32 devices in a mesh: rep: 2 (over x), fsdp: 16 (over z, y, core).
Axes of the slice: x: 2, y: 2, z: 4, core: 2. Of those that a mesh axis runs over, the one named last changes fastest.
Arguments:
- tokens: bfloat16 [256, 3584], P(('rep', 'fsdp')), may hold values from -6 to 6
- targets: bfloat16 [256, 3584], P(('rep', 'fsdp')), may hold values from -6 to 6
- gate_weight: bfloat16 [3584, 18944], P(None, 'fsdp'), may hold values from -0.09375 to 0.09375
- up_weight: bfloat16 [3584, 18944], P(None, 'fsdp'), may hold values from -0.09375 to 0.09375
- down_weight: bfloat16 [18944, 3584], P('fsdp'), may hold values from -0.046875 to 0.046875
- gate_direction: bfloat16 [3584, 18944], P(None, 'fsdp'), may hold values from -0.09375 to 0.09375
- up_direction: bfloat16 [3584, 18944], P(None, 'fsdp'), may hold values from -0.09375 to 0.09375
- down_direction: bfloat16 [18944, 3584], P('fsdp'), may hold values from -0.046875 to 0.046875
Outputs:
- hvp_gate: float32 [3584, 18944], P(None, 'fsdp')
- hvp_up: float32 [3584, 18944], P(None, 'fsdp')
- hvp_down: float32 [18944, 3584], P('fsdp')
The draws below stay inside these ranges and needn't reach their ends.
All inputs are finite; a program needn't handle non-finite values.
Results may differ from the reference program's by a relative error of at most 0.0069.
Values may be sent and summed in bfloat16 or wider, within the bound.
No kernel may reach another device: no remote copies, remote signals or barrier semaphores. Data moves between devices by JAX's collectives and lax.ppermute only.
A program may use at most 192 MiB of HBM per device.

```python
import jax
import jax.numpy as jnp
from jax import lax

D = 3584
FF = 18944
TOKENS = 256


def block_scale(key, extent, pieces, least, top_value):
    def one(position, shards_of):
        steps = jax.random.uniform(jax.random.fold_in(jax.random.fold_in(key, 6), position), (shards_of,), jnp.float32, least / len(pieces), top_value / len(pieces))
        return jnp.repeat(jnp.exp(steps), extent[position] // shards_of).reshape((-1,) + (1,) * (len(extent) - position - 1))

    level = one(*pieces[0])
    for cut in pieces[1:]:
        level = level * one(*cut)
    return level


def bell_draw(own_key, shape, spread, limit, shards=(), kind=jnp.bfloat16):
    factor_of = block_scale(own_key, shape, shards, -0.22, 0.18) if shards else 1.0
    entries = jax.random.normal(own_key, shape, jnp.float32) * spread * factor_of
    return jnp.minimum(jnp.maximum(entries, -limit), limit).astype(kind)


def setup_inputs(seed: int = 0) -> dict:
    streams_of = jax.random.split(jax.random.key(seed), 9)
    return {
        "tokens": bell_draw(streams_of[0], (TOKENS, D), 1.0, 6.0, ((0, 32),)),
        "targets": bell_draw(streams_of[1], (TOKENS, D), 1.0, 6.0, ((0, 32),)),
        "gate_weight": bell_draw(streams_of[2], (D, FF), D ** -0.5, 0.09375, ((1, 16),)),
        "up_weight": bell_draw(streams_of[3], (D, FF), D ** -0.5, 0.09375, ((1, 16),)),
        "down_weight": bell_draw(streams_of[4], (FF, D), FF ** -0.5, 0.046875, ((0, 16),)),
        "gate_direction": bell_draw(streams_of[5], (D, FF), D ** -0.5, 0.09375, ((1, 16),)),
        "up_direction": bell_draw(streams_of[6], (D, FF), D ** -0.5, 0.09375, ((1, 16),)),
        "down_direction": bell_draw(streams_of[7], (FF, D), FF ** -0.5, 0.046875, ((0, 16),)),
    }


def silu_parts(gate):
    sigmoid_value = jax.nn.sigmoid(gate)
    slope = sigmoid_value * (1.0 + gate * (1.0 - sigmoid_value))
    bend = sigmoid_value * (1.0 - sigmoid_value) * (2.0 + gate * (1.0 - 2.0 * sigmoid_value))
    return gate * sigmoid_value, slope, bend


def inner_rows(left, right):
    return lax.dot_general(left, right, (((0,), (0,)), ((), ())), preferred_element_type=jnp.float32)


def reference(tokens, targets, gate_weight, up_weight, down_weight, gate_direction, up_direction, down_direction):
    gate = jnp.dot(tokens, gate_weight, preferred_element_type=jnp.float32)
    up = jnp.dot(tokens, up_weight, preferred_element_type=jnp.float32)
    gate_tangent = jnp.dot(tokens, gate_direction, preferred_element_type=jnp.float32)
    up_tangent = jnp.dot(tokens, up_direction, preferred_element_type=jnp.float32)
    activation, slope, bend = silu_parts(gate)
    hidden = (activation * up).astype(jnp.bfloat16)
    hidden_tangent = (slope * gate_tangent * up + activation * up_tangent).astype(jnp.bfloat16)
    output = jnp.dot(hidden, down_weight, preferred_element_type=jnp.float32)
    output_tangent = jnp.dot(hidden_tangent, down_weight, preferred_element_type=jnp.float32) + jnp.dot(hidden, down_direction, preferred_element_type=jnp.float32)
    error = (output - targets.astype(jnp.float32)).astype(jnp.bfloat16)
    error_tangent = output_tangent.astype(jnp.bfloat16)
    back = jnp.dot(error, down_weight.T, preferred_element_type=jnp.float32)
    back_tangent = jnp.dot(error_tangent, down_weight.T, preferred_element_type=jnp.float32) + jnp.dot(error, down_direction.T, preferred_element_type=jnp.float32)
    gate_grad_tangent = (back_tangent * up * slope + back * up_tangent * slope + back * up * bend * gate_tangent).astype(jnp.bfloat16)
    up_grad_tangent = (back_tangent * activation + back * slope * gate_tangent).astype(jnp.bfloat16)
    hvp_gate = inner_rows(tokens, gate_grad_tangent)
    hvp_up = inner_rows(tokens, up_grad_tangent)
    hvp_down = inner_rows(hidden_tangent, error) + inner_rows(hidden, error_tangent)
    return hvp_gate, hvp_up, hvp_down
```

```python
import itertools

import jax
import jax.numpy as jnp
from jax import lax
from jax.experimental import pallas as pl
from jax.experimental.pallas import tpu as pltpu
from jax.sharding import PartitionSpec as P


F32 = jnp.float32
BF16 = jnp.bfloat16


def dot(left, right):
    return jnp.dot(left, right, preferred_element_type=F32)


def dot_t(left, right):
    return lax.dot_general(left, right, (((1,), (1,)), ((), ())), preferred_element_type=F32)


VMEM = pl.BlockSpec(memory_space=pltpu.VMEM)


def in_hbm(x):
    return pltpu.with_memory_space_constraint(x, pltpu.HBM)


def params(mib):
    return pltpu.CompilerParams(
        dimension_semantics=("arbitrary",), vmem_limit_bytes=mib * 1024 * 1024
    )


def block_rows(rows, steps):
    return pl.cdiv(pl.cdiv(rows, steps), 8) * 8


def rows_spec(rows, cols):
    return pl.BlockSpec((rows, cols), lambda i: (i, 0))


def sds(shape, dtype):
    return jax.ShapeDtypeStruct(shape, dtype)


def forward(toks, weights):
    gate, up, gt, ut = (dot_t(w, t) for w, t in zip(weights, toks))
    s = jax.nn.sigmoid(gate)
    act = gate * s
    slope = s * (1.0 + gate * (1.0 - s))
    bend = s * (1.0 - s) * (2.0 + gate * (1.0 - 2.0 * s))
    h = (act * up).astype(BF16)
    ht = (slope * gt * up + act * ut).astype(BF16)
    return up * slope, ut * slope + up * bend * gt, act, slope * gt, h, ht


def prefetch_body(pieces, src, dst, sem):
    n = src.shape[1] // pieces
    copies = [
        pltpu.make_async_copy(
            src.at[:, pl.ds(k * n, n)], dst.at[:, pl.ds(k * n, n)], sem.at[k]
        )
        for k in range(pieces)
    ]
    for c in copies:
        c.start()
    for c in copies:
        c.wait()


def prefetch(x, pieces=4):
    return pl.pallas_call(
        lambda *refs: prefetch_body(pieces, *refs),
        in_specs=[pl.BlockSpec(memory_space=pltpu.HBM)],
        out_specs=VMEM,
        out_shape=pltpu.VMEM(x.shape, x.dtype),
        scratch_shapes=[pltpu.SemaphoreType.DMA((pieces,))],
        compiler_params=pltpu.CompilerParams(vmem_limit_bytes=1024 * 1024),
        cost_estimate=pl.CostEstimate(
            flops=4000000000, bytes_accessed=2 * x.size, transcendentals=0
        ),
        name="prefetch",
    )(x)


def after(x, *deps):
    return lax.optimization_barrier((x, *deps))[0]


def products_body(n, tok, e, et, ggt, ugt, *refs):
    h, ht = side(refs[:n]), side(refs[n : 2 * n])
    o_gate, o_up, o_down = refs[2 * n :]
    t = tok[...]
    o_down[...] = dot(ht, e[...]) + dot(h, et[...])
    o_gate[...] = dot(ggt[...], t)
    o_up[...] = dot(ugt[...], t)


def side(refs):
    return jnp.concatenate([r[...] for r in refs], axis=1)


def products(tok, e, et, ggt, ugt, h, ht, bd=512):
    m, d = e.shape
    ff = ggt.shape[0]
    col = lambda rows: pl.BlockSpec((rows, bd), lambda j: (0, j))
    n = len(h)
    return pl.pallas_call(
        lambda *refs: products_body(n, *refs),
        grid=(d // bd,),
        in_specs=[col(m)] * 3 + [VMEM] * (2 + 2 * n),
        out_specs=[col(ff)] * 3,
        out_shape=[sds((ff, d), F32)] * 3,
        compiler_params=params(48),
        cost_estimate=pl.CostEstimate(
            flops=8 * m * d * ff, bytes_accessed=12 * d * ff, transcendentals=0
        ),
        name="products",
    )(tok, e, et, ggt, ugt, *h, *ht)


def dot_0(left, right):
    return lax.dot_general(left, right, (((0,), (0,)), ((), ())), preferred_element_type=F32)


def plan_of(fsdp):
    bits = [1 << b for b in range(fsdp.bit_length() - 1)]
    core, near, far = bits[:1], bits[1:2], bits[2:]
    groups = [[b] for b in far[::-1]]
    return core, near, groups


def masks(group):
    out = []
    for r in range(1, len(group) + 1):
        for c in itertools.combinations(group, r):
            out.append(sum(c))
    return sorted(out)


def make(mesh):
    rep, fsdp = mesh.shape["rep"], mesh.shape["fsdp"]
    core, near, far = plan_of(fsdp)

    def flip(x, mask):
        return lax.ppermute(x, "fsdp", [(i, i ^ mask) for i in range(fsdp)])

    def swap(x, mask):
        return lax.ppermute(x, "rep", [(i, i ^ mask) for i in range(rep)])

    rep_masks = list(range(1, rep))

    def spread(value, send, group):
        x, ids = value
        parts, all_ids = [x], list(ids)
        for m in group:
            parts.append(send(x, m))
            all_ids += [i ^ m if send is flip else i + m * fsdp for i in ids]
        return (jnp.concatenate(parts, axis=0), all_ids)

    def gather(x, stages, log):
        value = (x, [0])
        for send, group in stages:
            value = spread(value, send, group)
            log.append(value[0])
        return value

    def order(value, want):
        x, ids = value
        if ids == want:
            return x
        n = x.shape[0] // len(ids)
        return jnp.concatenate([x[ids.index(w) * n : (ids.index(w) + 1) * n] for w in want], axis=0)

    far_stages = [(flip, masks(g)) for g in far]
    near_stage = (flip, masks(near))
    core_stage = (flip, masks(core))
    rep_stage = (swap, rep_masks)

    def scatter(keep, send, ids, bits):
        n = keep.shape[0] // len(ids)
        got = flip(send, core[0])
        acc = keep + got.astype(F32)
        pieces = {i: acc[k * n : (k + 1) * n] for k, i in enumerate(ids)}
        for bit in bits:
            kept = [i for i in pieces if not i & bit]
            buf = jnp.concatenate([pieces[i | bit] for i in kept], axis=0).astype(BF16)
            got = flip(buf, bit)
            pieces = {
                i: pieces[i] + got[k * n : (k + 1) * n].astype(F32) for k, i in enumerate(kept)
            }
        return pieces[0]

    near_bits, far_bits = near, [g[0] for g in far][::-1]

    def on_device(tokens, targets, wg, wu, wd, dg, du, dd):
        weights = (wg.T, wu.T, dg.T, du.T)
        log = []
        mine = gather(tokens, far_stages + [near_stage], log)
        ids = mine[1]
        first_weights = (prefetch(after(weights[0], log[0])),) + weights[1:]
        tok_own, own_ids = spread(mine, *core_stage)
        got = [swap(mine[0], m) for m in rep_masks]
        half = tok_own.shape[0] // 2

        sets = [forward([tok_own] * 4, first_weights)]
        h1, ht1 = sets[0][4:]
        primal = dot_0(h1, wd)
        p_send = primal[half:].astype(BF16)
        h2, ht2 = after(h1, p_send), after(ht1, p_send)
        tangent = dot_0(ht2, wd) + dot_0(h2, dd)
        t_send = tangent[half:].astype(BF16)
        p_sum = scatter(primal[:half], p_send, ids, near_bits + far_bits)
        t_sum = scatter(tangent[:half], t_send, ids, far_bits[:1] + near_bits + far_bits[1:])
        error = (p_sum - targets.astype(F32)).astype(BF16)
        error_t = t_sum.astype(BF16)
        p_log, t_log = [], []
        p_val = gather(error, far_stages + [near_stage, rep_stage, core_stage], p_log)
        t_val = gather(error_t, [rep_stage] + far_stages + [near_stage, core_stage], t_log)
        toks, want = [tok_own], list(own_ids)
        for m, g in zip(rep_masks, got):
            full, fids = spread((g, ids), *core_stage)
            toks.append(full)
            want += [i + m * fsdp for i in fids]
            late = [after(full, x) for x in (error_t, t_log[0], t_log[1], t_log[2])]
            sets.append(forward(late, weights))
        a, b, act, c, h, ht = (list(x) for x in zip(*sets))
        tok = jnp.concatenate(toks, axis=0)
        e = order(p_val, want)
        et = order(t_val, want)
        a, b, act, c = (jnp.concatenate(x, axis=1) for x in (a, b, act, c))
        back = dot_t(wd, e)
        bt0 = dot_t(dd, e)
        bt = bt0 + dot_t(wd, et)
        ggt = (bt * a + back * b).astype(BF16)
        ugt = (bt * act + back * c).astype(BF16)
        gate_t, up_t, hvp_down = products(tok, e, et, ggt, ugt, h, ht)
        return gate_t.T, up_t.T, hvp_down

    return on_device


def solution(mesh):
    rows, cols, hid = P(("rep", "fsdp"), None), P(None, "fsdp"), P("fsdp", None)
    return jax.shard_map(
        make(mesh),
        mesh=mesh,
        in_specs=(rows, rows, cols, cols, hid, cols, cols, hid),
        out_specs=(cols, cols, hid),
        check_vma=False,
    )
```
